32 devices in a mesh: src: 16 (over z, y, x), hid: 2 (over core).
Axes of the slice: x: 2, y: 2, z: 4, core: 2. Of those that a mesh axis runs over, the one named last changes fastest.
Arguments:
- source_field: float32 [128, 2, 98, 128], P('src'), may hold values from -36 to 36
- hidden_gain: float32 [98], replicated, may hold values from 0.1 to 1.9
- enc_tiles: float32 [1024, 128, 128], P(('src', 'hid')), may hold values from -0.25 to 0.25
- enc_src_block: int32 [1024], P(('src', 'hid')), may hold values from 0 to 127, as said below
- enc_hid_block: int32 [1024], P(('src', 'hid')), may hold values from 0 to 63, as said below
- enc_count: int32 [32], P(('src', 'hid')), may hold values from 1 to 32, as said below
- dec_tiles: float32 [1024, 128, 128], P(('src', 'hid')), may hold values from -0.15625 to 0.15625
- dec_src_block: int32 [1024], P(('src', 'hid')), may hold values from 0 to 127, as said below
- dec_hid_block: int32 [1024], P(('src', 'hid')), may hold values from 0 to 63, as said below
- dec_count: int32 [32], P(('src', 'hid')), may hold values from 1 to 32, as said below
Outputs:
- returned: float32 [128, 2, 98, 128], P('src')
- channel_rms: float32 [98], replicated
The draws below stay inside these ranges and needn't reach their ends.
Inputs may be any that keep to these rules, and one draw needn't show every extreme that they name: `enc_src_block`: the 32 entries starting at (s * 2 + h) * 32 lie in s * 8 to (s + 1) * 8 - 1. `enc_hid_block`: the 32 entries starting at (s * 2 + h) * 32 lie in h * 32 to (h + 1) * 32 - 1; within these entries no pair (enc_src_block, enc_hid_block) repeats. `enc_count`: entry s * 2 + h counts the live slots of that group; it equals 32 for some group. `dec_src_block`: the 32 entries starting at (s * 2 + h) * 32 lie in s * 8 to (s + 1) * 8 - 1. `dec_hid_block`: the 32 entries starting at (s * 2 + h) * 32 lie in h * 32 to (h + 1) * 32 - 1; within these entries no pair (dec_src_block, dec_hid_block) repeats. `dec_count`: entry s * 2 + h counts the live slots of that group; it equals 32 for some group.
All inputs are finite; a program needn't handle non-finite values.
Results may differ from the reference program's by a relative error of at most 0.0003.
Values sent between devices are 32-bit elements; how exact they have to be, the bound alone decides.
No kernel may reach another device: no remote copies, remote signals or barrier semaphores. Data moves between devices by JAX's collectives and lax.ppermute only.
A program may use at most 64 MiB of HBM per device.

```python
import math
import jax
import jax.numpy as jnp
from jax import lax

CH = 98
BATCH = 2
TILE = 128
SRC_BLK = 8
HID_BLK = 32
ENC_CAP = 32
DEC_CAP = 32
SRC_BLOCKS = 128
HID_BLOCKS = 64
N_SRC = 16
N_HID = 2
DEVICES = 32


def block_pairs(key, salt, capacity):
    keys = jax.random.split(jax.random.fold_in(key, salt), DEVICES)

    def shuffle(one_key):
        return jax.random.permutation(one_key, SRC_BLK * HID_BLK)
    order = jax.vmap(shuffle)(keys)[:, :capacity].astype(jnp.int32)
    device = jnp.arange(DEVICES, dtype=jnp.int32)[:, None]
    src_base = device // N_HID * SRC_BLK
    hid_base = device % N_HID * HID_BLK
    return ((src_base + order // HID_BLK).reshape(-1), (hid_base + order % HID_BLK).reshape(-1))


def tile_counts(key, salt, capacity):
    first, second, third = jax.random.split(jax.random.fold_in(key, salt), 3)
    device = jnp.arange(DEVICES, dtype=jnp.int32)
    src_index = device // N_HID
    edge = max(1, N_SRC // 8)
    polar = (src_index < edge) | (src_index >= N_SRC - edge)
    heavy = jax.random.randint(first, (DEVICES,), capacity // 2, capacity + 1)
    light = jax.random.randint(second, (DEVICES,), 1, capacity // 4 + 1)
    counts = jnp.where(polar, heavy, light)
    fullest = jax.random.randint(third, (), 0, DEVICES)
    return counts.at[fullest].set(capacity).astype(jnp.int32)


def draw_source_field(key, part):
    first, second = jax.random.split(key, 2)
    shape = (SRC_BLOCKS, BATCH, CH, TILE)
    position = jnp.arange(SRC_BLOCKS, dtype=jnp.float32) / max(SRC_BLOCKS - 1, 1)
    channel = jnp.exp(jax.random.uniform(second, (CH,), jnp.float32, math.log(0.3), math.log(3.0)))
    ramp = 0.3 * 10.0 ** position
    noise = jnp.clip(jax.random.normal(first, shape, jnp.float32), -4.0, 4.0)
    return ramp[:, None, None, None] * channel[None, None, :, None] * noise


def draw_enc_src_block(key, part):
    return block_pairs(key, 11, ENC_CAP)[0]


def draw_enc_hid_block(key, part):
    return block_pairs(key, 11, ENC_CAP)[1]


def draw_enc_count(key, part):
    return tile_counts(key, 31, ENC_CAP)


def draw_dec_src_block(key, part):
    return block_pairs(key, 23, DEC_CAP)[0]


def draw_dec_hid_block(key, part):
    return block_pairs(key, 23, DEC_CAP)[1]


def draw_dec_count(key, part):
    return tile_counts(key, 37, DEC_CAP)


def steps_of(key, extent, cuts, smallest, largest):
    level = 1.0
    for dim, parts in cuts:
        heights = jax.random.uniform(jax.random.fold_in(jax.random.fold_in(key, 6), dim), (parts,), jnp.float32, smallest / len(cuts), largest / len(cuts))
        level = level * jnp.repeat(jnp.exp(heights), extent[dim] // parts).reshape((-1,) + (1,) * (len(extent) - 1 - dim))
    return level


def centred(key, extent, scale, limit, cuts=(), held_as=jnp.bfloat16):
    entries = scale * jax.random.normal(key, extent, jnp.float32)
    if cuts:
        entries = entries * steps_of(key, extent, cuts, -0.22, 0.18)
    return jnp.clip(entries, -limit, limit).astype(held_as)


def setup_inputs(seed: int = 0) -> dict:
    key_list = jax.random.split(jax.random.key(seed), 11)
    source_field = draw_source_field(jax.random.fold_in(key_list[10], 71), 0)
    hidden_gain = jnp.clip(1.0 + 0.18 * jax.random.normal(key_list[1], (CH,), jnp.float32), 0.1, 1.9)
    enc_tiles = centred(key_list[2], (DEVICES * ENC_CAP, TILE, TILE), (4 * TILE) ** -0.5, 0.25, ((0, 32),), jnp.float32)
    enc_src_block = draw_enc_src_block(jax.random.fold_in(key_list[10], 71), 0)
    enc_hid_block = draw_enc_hid_block(jax.random.fold_in(key_list[10], 71), 0)
    enc_count = draw_enc_count(jax.random.fold_in(key_list[10], 71), 0)
    dec_tiles = centred(key_list[6], (DEVICES * DEC_CAP, TILE, TILE), (12 * TILE) ** -0.5, 0.15625, ((0, 32),), jnp.float32)
    dec_src_block = draw_dec_src_block(jax.random.fold_in(key_list[10], 71), 0)
    dec_hid_block = draw_dec_hid_block(jax.random.fold_in(key_list[10], 71), 0)
    dec_count = draw_dec_count(jax.random.fold_in(key_list[10], 71), 0)
    return {"source_field": source_field, "hidden_gain": hidden_gain, "enc_tiles": enc_tiles, "enc_src_block": enc_src_block, "enc_hid_block": enc_hid_block, "enc_count": enc_count, "dec_tiles": dec_tiles, "dec_src_block": dec_src_block, "dec_hid_block": dec_hid_block, "dec_count": dec_count}


HIGH = lax.Precision.HIGHEST

def remap(values, tiles, from_block, to_block, counts, out_blocks, capacity):
    slots = jnp.arange(capacity, dtype=jnp.int32)

    def one_device(total, inputs):
        tile_set, sources, targets, live_count = inputs
        blocks = jnp.take(values, sources, axis=0)
        product = jnp.einsum('tfr,trc->tfc', blocks, tile_set, precision=HIGH)
        keep = (slots < live_count).astype(values.dtype)
        return (total.at[targets].add(product * keep[:, None, None]), None)
    start = jnp.zeros((out_blocks, values.shape[1], values.shape[2]), values.dtype)
    inputs = (tiles.reshape(-1, capacity, tiles.shape[1], tiles.shape[2]), from_block.reshape(-1, capacity), to_block.reshape(-1, capacity), counts)
    total, unused = lax.scan(one_device, start, inputs)
    return total

def normalize(total, gain, batch, channels):
    nodes, features, width = total.shape
    grouped = total.reshape(nodes, batch, channels, width)
    mean_square = lax.optimization_barrier(jnp.mean(grouped * grouped, axis=2, keepdims=True))
    scaled = grouped * gain[None, None, :, None] * lax.rsqrt(mean_square + 1e-06)
    return scaled.reshape(nodes, features, width)

def reference(source_field, hidden_gain, enc_tiles, enc_src_block, enc_hid_block, enc_count, dec_tiles, dec_src_block, dec_hid_block, dec_count):
    blocks, batch, channels, width = source_field.shape
    flat = source_field.reshape(blocks, batch * channels, width)
    hidden_sum = remap(flat, enc_tiles, enc_src_block, enc_hid_block, enc_count, HID_BLOCKS, ENC_CAP)
    hidden = normalize(hidden_sum, hidden_gain, batch, channels)
    returned = remap(hidden, dec_tiles, dec_hid_block, dec_src_block, dec_count, SRC_BLOCKS, DEC_CAP)
    returned = returned.reshape(source_field.shape)
    difference = returned - source_field
    channel_rms = jnp.sqrt(lax.optimization_barrier(jnp.mean(difference * difference, axis=(0, 1, 3))) + 1e-06)
    return (returned, channel_rms)
```

```python
import functools

import jax
import jax.numpy as jnp
from jax import lax
from jax.experimental import pallas as pl
from jax.experimental.pallas import tpu as pltpu
from jax.sharding import PartitionSpec as P

HID_BLK = 32
EPSILON = 1e-06

VMEM = pltpu.MemorySpace.VMEM
SMEM = pltpu.MemorySpace.SMEM


def row_count(rows):
    return (rows + 7) // 8 * 8


def bit_orders(bits, streams):
    return [bits[s % len(bits):] + bits[: s % len(bits)] for s in range(streams)]


def split(value):
    high = value.astype(jnp.bfloat16)
    low = (value - high.astype(jnp.float32)).astype(jnp.bfloat16)
    return high, low


def tile_weights(tile):
    high, low = split(tile)
    line = jnp.concatenate([high, low], axis=1)
    return jnp.concatenate([line, line], axis=0)


def block_rows(value):
    return jnp.concatenate(split(value), axis=1)


def multiply(rows, tile):
    product = jnp.dot(rows, tile_weights(tile), preferred_element_type=jnp.float32)
    width = tile.shape[1]
    return product[:, :width] + product[:, width:]


def position_of(block, mine, orders):
    streams = len(orders)
    stream = lax.rem(block, streams)
    away = lax.bitwise_xor(lax.div(block, streams), mine)
    depth = len(orders[0])
    spot = jnp.int32(0)
    for s, order in enumerate(orders):
        value = jnp.int32(0)
        for stage, bit in enumerate(order):
            one = lax.bitwise_and(lax.shift_right_logical(away, bit), 1)
            value = value + one * (1 << (depth - 1 - stage))
        spot = jnp.where(stream == s, value, spot)
    return stream * (1 << depth) + spot


def encode_kernel(orders, unroll, count, sources, targets, field, tiles, *rest):
    streams = len(orders)
    outs, (lhs, acc, sems) = rest[: 2 * streams], rest[2 * streams:]
    blocks, batch, channels, width = field.shape
    rows = lhs.shape[1]
    size = 1 << len(orders[0])
    half = size // 2
    mine = lax.bitwise_and(lax.axis_index("src"), size - 1)
    pad = jnp.zeros((rows - batch * channels, width), jnp.float32)
    for b in range(blocks):
        lhs[b] = block_rows(jnp.concatenate([field[b, n] for n in range(batch)] + [pad], axis=0))
    acc[...] = jnp.zeros_like(acc)
    live = count[0]

    def step(group, carry):
        for u in range(unroll):
            k = group * unroll + u
            product = multiply(lhs[lax.rem(sources[k], blocks)], tiles[k])
            place = position_of(lax.rem(targets[k], HID_BLK), mine, orders)
            acc[place] += jnp.where(k < live, product, 0.0)
        return carry

    lax.fori_loop(0, lax.div(live + unroll - 1, unroll), step, 0)
    copies = []
    for s in range(streams):
        for part, start in ((0, half), (1, 0)):
            copies.append(pltpu.make_async_copy(
                acc.at[pl.ds(s * size + start, half)], outs[2 * s + part], sems.at[2 * s + part]))
    for copy in copies:
        copy.start()
    for copy in copies:
        copy.wait()


def normalize_kernel(batch, channels, mine, other, gain, out):
    total = mine[...] + other[...]
    row = lax.broadcasted_iota(jnp.int32, total.shape, 1)
    square = total * total
    scale = jnp.zeros_like(total)
    for n in range(batch):
        inside = (row >= n * channels) & (row < (n + 1) * channels)
        mean = jnp.sum(jnp.where(inside, square, 0.0), axis=1, keepdims=True) / channels
        scale = jnp.where(inside, lax.rsqrt(mean + EPSILON), scale)
    out[...] = total * gain[...] * scale


def decode_kernel(orders, unroll, count, targets, sources, tiles, *rest):
    streams = len(orders)
    hidden, out, lhs = rest[: 2 * streams], rest[2 * streams], rest[2 * streams + 1]
    blocks = out.shape[0]
    size = 1 << len(orders[0])
    half = size // 2
    mine = lax.bitwise_and(lax.axis_index("src"), size - 1)
    for s in range(streams):
        for part in range(2):
            for i in range(half):
                lhs[s * size + part * half + i] = block_rows(hidden[2 * s + part][i])
    out[...] = jnp.zeros_like(out)
    live = count[0]

    def step(group, carry):
        for u in range(unroll):
            k = group * unroll + u
            place = position_of(lax.rem(sources[k], HID_BLK), mine, orders)
            product = multiply(lhs[place], tiles[k])
            out[lax.rem(targets[k], blocks)] += jnp.where(k < live, product, 0.0)
        return carry

    lax.fori_loop(0, lax.div(live + unroll - 1, unroll), step, 0)


def finish_kernel(field, mine, other, out, sums):
    blocks, batch, channels, width = field.shape
    square = jnp.zeros((channels, width), jnp.float32)
    for b in range(blocks):
        total = mine[b] + other[b]
        for n in range(batch):
            part = total[n * channels:(n + 1) * channels]
            out[b, n] = part
            error = part - field[b, n]
            square = square + error * error
    sums[...] = lax.dot_general(
        jnp.ones((8, width), jnp.float32), square, (((1,), (1,)), ((), ())),
        precision=lax.Precision.HIGHEST, preferred_element_type=jnp.float32)


def flip(value, axis, mask, count):
    return lax.ppermute(value, axis, [(i, i ^ mask) for i in range(count)])


def body(
    source_field,
    hidden_gain,
    enc_tiles,
    enc_src_block,
    enc_hid_block,
    enc_count,
    dec_tiles,
    dec_src_block,
    dec_hid_block,
    dec_count,
):
    src_blocks, batch, channels, width = source_field.shape
    n_src = lax.axis_size("src")
    n_hid = lax.axis_size("hid")
    levels = n_src.bit_length() - 1
    bits = list(range(levels - 1))
    cube = 1 << len(bits)
    streams = HID_BLK // cube
    half = cube // 2
    orders = bit_orders(bits, streams)
    rows = row_count(batch * channels)
    slots = enc_tiles.shape[0]
    unroll = 4
    smem, vmem = pl.BlockSpec(memory_space=SMEM), pl.BlockSpec(memory_space=VMEM)
    anywhere = pl.BlockSpec(memory_space=pl.ANY)
    shape = lambda *dims: jax.ShapeDtypeStruct(dims, jnp.float32)
    params = pltpu.CompilerParams(vmem_limit_bytes=48 * 1024 * 1024)

    gain = jnp.concatenate([jnp.tile(hidden_gain, batch), jnp.zeros((rows - batch * channels,))])
    gain = jnp.broadcast_to(gain[None, :, None], (1, rows, width))

    pieces = pl.pallas_call(
        functools.partial(encode_kernel, orders, unroll),
        out_shape=[shape(half, rows, width)] * (2 * streams),
        in_specs=[smem, smem, smem, vmem, vmem],
        out_specs=[anywhere] * (2 * streams),
        scratch_shapes=[
            pltpu.VMEM((src_blocks, rows, 2 * width), jnp.bfloat16),
            pltpu.VMEM((HID_BLK, rows, width), jnp.float32),
            pltpu.SemaphoreType.DMA((2 * streams,)),
        ],
        compiler_params=params,
        name="encode",
    )(enc_count, enc_src_block, enc_hid_block, source_field, enc_tiles)

    send = [pieces[2 * s] for s in range(streams)]
    keep = [pieces[2 * s + 1] for s in range(streams)]
    for stage in range(len(bits)):
        came = [flip(send[s], "src", 1 << orders[s][stage], n_src) for s in range(streams)]
        for s in range(streams):
            upper = half >> (stage + 1)
            if upper:
                send[s] = keep[s][upper:] + came[s][upper:]
                keep[s] = keep[s][:upper] + came[s][:upper]
            else:
                keep[s] = keep[s] + came[s]
    came = [flip(keep[s], "src", cube, n_src) for s in range(streams)]
    hidden = []
    for s in range(streams):
        hidden.append(pl.pallas_call(
            functools.partial(normalize_kernel, batch, channels),
            out_shape=shape(1, rows, width),
            in_specs=[vmem] * 3,
            out_specs=vmem,
            name="normalize",
        )(keep[s], came[s], gain))
    upper = [None] * streams
    for stage in reversed(range(len(bits))):
        came = [flip(hidden[s], "src", 1 << orders[s][stage], n_src) for s in range(streams)]
        for s in range(streams):
            if stage:
                hidden[s] = jnp.concatenate([hidden[s], came[s]], axis=0)
            else:
                upper[s] = came[s]
    halves = []
    for s in range(streams):
        halves += [hidden[s], upper[s]]

    partial_back = pl.pallas_call(
        functools.partial(decode_kernel, orders, unroll),
        out_shape=shape(src_blocks, rows, width),
        in_specs=[smem, smem, smem, vmem] + [vmem] * (2 * streams),
        out_specs=vmem,
        scratch_shapes=[pltpu.VMEM((HID_BLK, rows, 2 * width), jnp.bfloat16)],
        compiler_params=params,
        name="decode",
    )(dec_count, dec_src_block, dec_hid_block, dec_tiles, *halves)

    if n_hid == 2:
        others = flip(partial_back, "hid", 1, n_hid)
    else:
        others = jnp.zeros_like(partial_back)
        partial_back = lax.psum(partial_back, "hid")
    returned, sums = pl.pallas_call(
        finish_kernel,
        out_shape=[shape(*source_field.shape), shape(8, channels)],
        in_specs=[vmem] * 3,
        out_specs=[vmem] * 2,
        compiler_params=params,
        name="finish",
    )(source_field, partial_back, others)

    for low in range(0, levels, 2):
        masks = [1 << low]
        if low + 1 < levels:
            masks += [2 << low, 3 << low]
        came = [flip(sums, "src", mask, n_src) for mask in masks]
        sums = sums + came[0]
        if len(came) == 3:
            sums = sums + (came[1] + came[2])
    total_points = src_blocks * n_src * batch * width
    channel_rms = jnp.sqrt(sums[0] / total_points + EPSILON)
    return (returned, channel_rms)


def solution(mesh):
    in_specs = (
        P("src", None, None, None),
        P(),
        P(("src", "hid"), None, None),
        P(("src", "hid")),
        P(("src", "hid")),
        P(("src", "hid")),
        P(("src", "hid"), None, None),
        P(("src", "hid")),
        P(("src", "hid")),
        P(("src", "hid")),
    )
    out_specs = (P("src", None, None, None), P())
    return jax.shard_map(body, mesh=mesh, in_specs=in_specs, out_specs=out_specs, check_vma=False)
```

```python
import functools

import jax
import jax.numpy as jnp
from jax import lax
from jax.experimental import pallas as pl
from jax.experimental.pallas import tpu as pltpu
from jax.sharding import PartitionSpec as P

HID_BLK = 32
EPSILON = 1e-06
UNROLL = 4

VMEM = pltpu.MemorySpace.VMEM
SMEM = pltpu.MemorySpace.SMEM
IN_VMEM = pl.BlockSpec(memory_space=VMEM)
IN_SMEM = pl.BlockSpec(memory_space=SMEM)
ANYWHERE = pl.BlockSpec(memory_space=pl.ANY)
PARAMS = pltpu.CompilerParams(vmem_limit_bytes=24 * 1024 * 1024)


class Stream:
    def __init__(self, first, units, orders):
        self.first, self.units, self.orders = first, units, orders


def make_streams(bits, owned):
    turn = lambda k: bits[k % len(bits):] + bits[: k % len(bits)]
    streams = []
    for unit in range(owned):
        first = unit % len(bits)
        second = first + (unit + 1 == owned and owned > len(bits))
        streams.append(Stream(unit, 1, (turn(first), turn(second))))
    return streams


def split(value):
    high = value.astype(jnp.bfloat16)
    low = (value - high.astype(jnp.float32)).astype(jnp.bfloat16)
    return high, low


def tile_weights(tile):
    high, low = split(tile)
    line = jnp.concatenate([high, low], axis=1)
    return jnp.concatenate([line, line], axis=0)


def block_rows(value):
    return jnp.concatenate(split(value), axis=1)


def multiply(rows, tile):
    product = jnp.dot(rows, tile_weights(tile), preferred_element_type=jnp.float32)
    width = tile.shape[1]
    return product[:, :width] + product[:, width:]


def position_of(block, cube, streams):
    mine = lax.bitwise_and(lax.axis_index("src"), cube - 1)
    core = lax.bitwise_and(lax.axis_index("hid"), 1)
    away = lax.bitwise_xor(lax.rem(block, cube), mine)
    unit = lax.div(block, cube)
    place = jnp.int32(0)
    for stream in streams:
        depth = len(stream.orders[0])
        spot = jnp.int32(0)
        for stage in range(depth):
            bit = jnp.where(core == 0, stream.orders[0][stage], stream.orders[1][stage])
            one = lax.bitwise_and(lax.shift_right_logical(away, bit), 1)
            spot = spot + one * (1 << (depth - 1 - stage))
        here = stream.first * cube + spot * stream.units + unit - stream.first
        place = jnp.where(unit >= stream.first, here, place)
    return place


def encode_kernel(cube, streams, count, sources_in, targets_in, field_in, tiles_in, *rest):
    outs = rest[: 2 * len(streams)]
    sources, targets, field, tiles, lhs, acc, small, large, sems = rest[2 * len(streams):]
    blocks, rows = lhs.shape[0], lhs.shape[1]
    used = field.shape[0] // blocks
    groups = tiles.shape[0] // UNROLL
    copies = [pltpu.make_async_copy(sources_in, sources, small.at[1]),
              pltpu.make_async_copy(targets_in, targets, small.at[2]),
              pltpu.make_async_copy(field_in, field, large)]

    def tile_copy(g):
        span = pl.ds(g * UNROLL, UNROLL)
        return pltpu.make_async_copy(tiles_in.at[span], tiles.at[span], sems.at[g])

    for copy in copies:
        copy.start()
    for g in range(groups):
        tile_copy(g).start()
    acc[...] = jnp.zeros_like(acc)
    for copy in copies:
        copy.wait()
    pad = jnp.zeros((rows - used, field.shape[1]), jnp.float32)
    for b in range(blocks):
        lhs[b] = block_rows(jnp.concatenate([field[b * used:(b + 1) * used], pad], axis=0))
    live = count[0]
    busy = lax.div(live + UNROLL - 1, UNROLL)

    def step(g, carry):
        tile_copy(g).wait()
        for u in range(UNROLL):
            k = g * UNROLL + u
            product = multiply(lhs[lax.rem(sources[k], blocks)], tiles[k])
            place = position_of(lax.rem(targets[k], HID_BLK), cube, streams)
            acc[place] += jnp.where(k < live, product, 0.0)
        return carry

    def drain(g, carry):
        tile_copy(g).wait()
        return carry

    lax.fori_loop(0, busy, step, 0)
    lax.fori_loop(busy, groups, drain, 0)
    half = cube // 2
    for s, stream in enumerate(streams):
        start, size = stream.first * cube, stream.units * half
        outs[2 * s][...] = acc[start + size:start + 2 * size]
        outs[2 * s + 1][...] = acc[start:start + size]


def fold_kernel(keep, came, send_out, keep_out):
    size = send_out.shape[0]
    send_out[...] = keep[size:] + came[size:]
    keep_out[...] = keep[:size] + came[:size]


def add_kernel(first, second, out):
    out[...] = first[...] + second[...]


def normalize_kernel(batch, channels, mine, other, gain, out):
    for i in range(out.shape[0]):
        total = mine[i] + other[i]
        row = lax.broadcasted_iota(jnp.int32, total.shape, 0)
        square = total * total
        scale = jnp.zeros_like(total)
        for n in range(batch):
            inside = lax.rem(row, batch) == n
            mean = jnp.sum(jnp.where(inside, square, 0.0), axis=0, keepdims=True) / channels
            scale = jnp.where(inside, lax.rsqrt(mean + EPSILON), scale)
        out[i] = total * gain[...] * scale


def join_kernel(first, second, out):
    size = first.shape[0]
    out[:size] = first[...]
    out[size:] = second[...]


def decode_kernel(cube, streams, count, targets, sources, tiles, *rest):
    hidden, out, lhs = rest[: 2 * len(streams)], rest[2 * len(streams)], rest[2 * len(streams) + 1]
    blocks = out.shape[0]
    half = cube // 2
    for s, stream in enumerate(streams):
        size = stream.units * half
        for part in range(2):
            for i in range(size):
                lhs[stream.first * cube + part * size + i] = block_rows(hidden[2 * s + part][i])
    out[...] = jnp.zeros_like(out)
    live = count[0]

    def step(g, carry):
        for u in range(UNROLL):
            k = g * UNROLL + u
            place = position_of(lax.rem(sources[k], HID_BLK), cube, streams)
            product = multiply(lhs[place], tiles[k])
            out[lax.rem(targets[k], blocks)] += jnp.where(k < live, product, 0.0)
        return carry

    lax.fori_loop(0, lax.div(live + UNROLL - 1, UNROLL), step, 0)


def finish_kernel(batch, field, mine, other, out, sums):
    blocks, _, width = mine.shape
    used = field.shape[0] // blocks
    square = jnp.zeros((used, width), jnp.float32)
    for b in range(blocks):
        total = (mine[b] + other[b])[:used]
        out[b * used:(b + 1) * used] = total
        error = total - field[b * used:(b + 1) * used]
        square = square + error * error
    high = lax.Precision.HIGHEST
    lanes = lax.dot_general(jnp.ones((8, width), jnp.float32), square, (((1,), (1,)), ((), ())),
                            precision=high, preferred_element_type=jnp.float32)
    row = lax.broadcasted_iota(jnp.int32, (used, width), 0)
    column = lax.broadcasted_iota(jnp.int32, (used, width), 1)
    pick = (lax.div(row, batch) == column).astype(jnp.float32)
    sums[...] = jnp.dot(lanes, pick, precision=high, preferred_element_type=jnp.float32)


def ORDER(depth, streams):
    return [(stage, s) for stage in range(2 * depth + 1) for s in range(streams)]


def flip(value, axes, partner, count):
    return lax.ppermute(value, axes, [(i, partner(i)) for i in range(count)])


def kernel(function, outs, scratch=(), specs=None):
    def call(*args):
        in_specs = specs or [IN_VMEM] * len(args)
        args = [pltpu.with_memory_space_constraint(a, pltpu.VMEM) if s is IN_VMEM else
                pltpu.with_memory_space_constraint(a, pltpu.HBM) if s is ANYWHERE else a
                for a, s in zip(args, in_specs)]
        return pl.pallas_call(
            function, out_shape=[pltpu.VMEM(o, jnp.float32) for o in outs], in_specs=in_specs,
            out_specs=[IN_VMEM] * len(outs), scratch_shapes=list(scratch),
            compiler_params=PARAMS)(*args)

    return call


def body(
    source_field,
    hidden_gain,
    enc_tiles,
    enc_src_block,
    enc_hid_block,
    enc_count,
    dec_tiles,
    dec_src_block,
    dec_hid_block,
    dec_count,
):
    src_blocks, batch, channels, width = source_field.shape
    n_src = lax.axis_size("src")
    n_hid = lax.axis_size("hid")
    levels = n_src.bit_length() - 1
    bits = list(range(levels - 1))
    cube = 1 << len(bits)
    half = cube // 2
    owned = HID_BLK // cube
    streams = make_streams(bits, owned)
    used = batch * channels
    rows = (used + 7) // 8 * 8
    slots = enc_tiles.shape[0]
    both = ("src", "hid")
    count = n_src * n_hid

    def swap(value, masks):
        def partner(i):
            src, hid = divmod(i, n_hid)
            return (src ^ masks[hid & 1]) * n_hid + hid

        return flip(value, both, partner, count)

    field = source_field.transpose(0, 2, 1, 3).reshape(src_blocks * used, width)
    gain = jnp.concatenate([jnp.repeat(hidden_gain, batch), jnp.zeros((rows - used,))])
    gain = jnp.broadcast_to(gain[:, None], (rows, width))

    pieces = kernel(
        functools.partial(encode_kernel, cube, streams),
        [(s.units * half, rows, width) for s in streams for _ in range(2)],
        specs=[IN_SMEM] + [ANYWHERE] * 4,
        scratch=[
            pltpu.SMEM((slots,), jnp.int32),
            pltpu.SMEM((slots,), jnp.int32),
            pltpu.VMEM((src_blocks * used, width), jnp.float32),
            pltpu.VMEM((slots, width, width), jnp.float32),
            pltpu.VMEM((src_blocks, rows, 2 * width), jnp.bfloat16),
            pltpu.VMEM((HID_BLK, rows, width), jnp.float32),
            pltpu.SemaphoreType.DMA((3,)),
            pltpu.SemaphoreType.DMA,
            pltpu.SemaphoreType.DMA((slots // UNROLL,)),
        ],
    )(enc_count, enc_src_block, enc_hid_block, field, enc_tiles)

    send = list(pieces[0::2])
    keep = list(pieces[1::2])
    hidden = [None] * len(streams)
    upper = [None] * len(streams)
    depth = len(bits)
    for stage, s in ORDER(depth, len(streams)):
        mask = (cube, cube) if stage == depth else tuple(
            1 << o[min(stage, 2 * depth - stage)] for o in streams[s].orders)
        if stage < depth:
            came = swap(send[s], mask)
            if stage + 1 < depth:
                size = keep[s].shape[0] // 2
                send[s], keep[s] = kernel(fold_kernel, [(size, rows, width)] * 2)(keep[s], came)
            else:
                [keep[s]] = kernel(add_kernel, [keep[s].shape])(keep[s], came)
        elif stage == depth:
            came = swap(keep[s], mask)
            [hidden[s]] = kernel(functools.partial(normalize_kernel, batch, channels), [keep[s].shape])(keep[s], came, gain)
        else:
            came = swap(hidden[s], mask)
            if stage < 2 * depth:
                [hidden[s]] = kernel(join_kernel, [(2 * hidden[s].shape[0], rows, width)])(
                    hidden[s], came)
            else:
                upper[s] = came

    [partial_back] = kernel(
        functools.partial(decode_kernel, cube, streams),
        [(src_blocks, rows, width)],
        specs=[IN_SMEM] * 3 + [IN_VMEM] * (1 + 2 * len(streams)),
        scratch=[pltpu.VMEM((HID_BLK, rows, 2 * width), jnp.bfloat16)],
    )(dec_count, dec_src_block, dec_hid_block, dec_tiles, *[x for pair in zip(hidden, upper) for x in pair])

    if n_hid == 2:
        others = flip(partial_back, "hid", lambda i: i ^ 1, n_hid)
    else:
        others = jnp.zeros_like(partial_back)
        partial_back = lax.psum(partial_back, "hid")
    returned, sums = kernel(
        functools.partial(finish_kernel, batch), [(src_blocks * used, width), (8, width)],
    )(field, partial_back, others)
    returned = returned.reshape(src_blocks, channels, batch, width).transpose(0, 2, 1, 3)

    for low in range(0, levels, 2):
        flips = [1 << low]
        if low + 1 < levels:
            flips += [2 << low, 3 << low]
        came = [flip(sums, "src", lambda i, mask=mask: i ^ mask, n_src) for mask in flips]
        sums = sums + came[0]
        if len(came) == 3:
            sums = sums + (came[1] + came[2])
    total_points = src_blocks * n_src * batch * width
    channel_rms = jnp.sqrt(sums[0, :channels] / total_points + EPSILON)
    return (returned, channel_rms)


def solution(mesh):
    in_specs = (
        P("src", None, None, None),
        P(),
        P(("src", "hid"), None, None),
        P(("src", "hid")),
        P(("src", "hid")),
        P(("src", "hid")),
        P(("src", "hid"), None, None),
        P(("src", "hid")),
        P(("src", "hid")),
        P(("src", "hid")),
    )
    out_specs = (P("src", None, None, None), P())
    return jax.shard_map(body, mesh=mesh, in_specs=in_specs, out_specs=out_specs, check_vma=False)
```
